32 devices in a mesh: dp: 4 (over y, core), seq: 2 (over x), head: 4 (over z).
Axes of the slice: x: 2, y: 2, z: 4, core: 2. Of those that a mesh axis runs over, the one named last changes fastest.
Arguments:
- queries: bfloat16 [4, 512, 1536], P('dp', 'seq', 'head'), may hold values from -160 to 160
- key_cache: bfloat16 [4, 512, 512], P('dp', 'seq', 'head'), may hold values from -7 to 7
- value_cache: bfloat16 [4, 512, 512], P('dp', 'seq', 'head'), may hold values from -6 to 6
- out_grad: bfloat16 [4, 512, 1536], P('dp', 'seq', 'head'), may hold values from -6 to 6
- doc_ids: int32 [4, 512], P('dp', 'seq'), may hold values from 0 to 1, never falling along the last dimension, each value on 1 to 511 neighbouring positions
- layer_input: bfloat16 [4, 512, 3072], P('dp', ('seq', 'head')), may hold values from -6 to 6
- key_proj: bfloat16 [3072, 512], P(None, 'head'), may hold values from -0.109375 to 0.109375
- value_proj: bfloat16 [3072, 512], P(None, 'head'), may hold values from -0.109375 to 0.109375
Outputs:
- query_grad: bfloat16 [4, 512, 1536], P('dp', 'seq', 'head')
- input_grad: bfloat16 [4, 512, 3072], P('dp', ('seq', 'head'))
- grad_keyproj: float32 [3072, 512], P(None, 'head')
- grad_valueproj: float32 [3072, 512], P(None, 'head')
The draws below stay inside these ranges and needn't reach their ends.
Inputs may be any that keep to these rules, and one draw needn't show every extreme that they name: `doc_ids`: document numbers never fall along a sequence; a document spans 1 to 511 positions.
All inputs are finite; a program needn't handle non-finite values.
Results may differ from the reference program's by a relative error of at most 0.02.
Values may be sent and summed in bfloat16 or wider, within the bound.
No kernel may reach another device: no remote copies, remote signals or barrier semaphores. Data moves between devices by JAX's collectives and lax.ppermute only.
A program may use at most 64 MiB of HBM per device.

```python
import math
import jax
import jax.numpy as jnp
import numpy as np
from jax import lax

D = 3072
HD = 128
GROUP = 3
KVH = 4
QH = 12
LEN = 512
SEQS = 4


def shared_draw(key):
    base_keys = jax.random.truncated_normal(jax.random.fold_in(key, 101), -6.0, 6.0, (SEQS, LEN, KVH * HD), jnp.float32)
    return base_keys


def draw_key_cache(key, part):
    base_keys = shared_draw(key)
    return base_keys.astype(jnp.bfloat16)


def draw_queries(key, part):
    base_query = jax.random.truncated_normal(jax.random.fold_in(key, 303), -6.0, 6.0, (SEQS, LEN, QH * HD), jnp.float32)
    return base_query.astype(jnp.bfloat16)


def levels(stream_key, dims, cuts, smallest, high):
    def one(axis_at, parts):
        steps = jax.random.uniform(jax.random.fold_in(jax.random.fold_in(stream_key, 6), axis_at), (parts,), jnp.float32, smallest / len(cuts), high / len(cuts))
        return jnp.repeat(jnp.exp(steps), dims[axis_at] // parts).reshape((-1,) + (1,) * (len(dims) - axis_at - 1))

    loudness = one(*cuts[0])
    for cut in cuts[1:]:
        loudness = loudness * one(*cut)
    return loudness


def profile(count, total, limit, slope):
    portions = [(1 << 20) // math.isqrt(grade ** slope) + 1 for grade in range(2, count + 1)]
    spare, given = total - limit - (count - 1), [1] * (count - 1)
    while spare > 0:
        free = [i for i in range(count - 1) if given[i] < limit]
        whole, left = sum([portions[i] for i in free]), spare
        for i in free:
            addition = min(limit - given[i], max(1, left * portions[i] // whole), spare)
            given[i] = given[i] + addition
            spare = spare - addition
    return np.array([limit] + given)


def uneven_parts(own_key, count, total, bound, slope):
    if count == 2:
        one = jax.random.randint(own_key, (), max(1, total - bound), min(bound, total - 1) + 1)
        return jnp.stack([one, total - one])
    sizes = jnp.asarray(profile(count, total, bound, slope), jnp.int32)
    couples = (count - 1) // 2
    source_of, receiver = sizes[1:1 + 2 * couples:2], sizes[2:2 + 2 * couples:2]
    room = jnp.minimum(source_of - 1, bound - receiver)
    shifted = jax.random.randint(jax.random.fold_in(own_key, 1), (couples,), 0, 1 << 20) % (room + 1)
    sizes = sizes.at[1:1 + 2 * couples:2].set(source_of - shifted).at[2:2 + 2 * couples:2].set(receiver + shifted)
    return sizes[jax.random.permutation(jax.random.fold_in(own_key, 2), count)]


def gaussian(own_key, extent, deviation, bound, pieces=(), kind=jnp.bfloat16):
    values = jax.random.normal(own_key, extent, jnp.float32) * deviation
    if len(pieces) > 0:
        values = levels(own_key, extent, pieces, -0.22, 0.18) * values
    return jnp.clip(values, min=-bound, max=bound).astype(kind)


def setup_inputs(seed: int = 0) -> dict:
    seeds = jax.random.split(jax.random.key(seed), 9)
    return {
        "queries": draw_queries(jax.random.fold_in(seeds[8], 71), 0),
        "key_cache": draw_key_cache(jax.random.fold_in(seeds[8], 71), 0),
        "value_cache": gaussian(seeds[2], (SEQS, LEN, KVH * HD), 1.0, 6.0, ((0, 4), (1, 2), (2, 4))),
        "out_grad": gaussian(seeds[3], (SEQS, LEN, QH * HD), 1.0, 6.0, ((0, 4), (1, 2), (2, 4))),
        "doc_ids": jax.vmap(lambda own: jnp.searchsorted(jnp.cumsum(uneven_parts(own, 2, LEN, LEN - 1, 0)), jnp.arange(LEN), side="right"))(jax.random.split(seeds[4], SEQS)).reshape((SEQS, LEN)).astype(jnp.int32),
        "layer_input": gaussian(seeds[5], (SEQS, LEN, D), 1.0, 6.0, ((0, 4), (1, 8))),
        "key_proj": gaussian(seeds[6], (D, KVH * HD), D ** -0.5, 0.109375, ((1, 4),)),
        "value_proj": gaussian(seeds[7], (D, KVH * HD), D ** -0.5, 0.109375, ((1, 4),)),
    }


NEG_FILL = -1e30


def head_grads(query_block, key_block, value_block, grad_block, doc_row):
    score_scale = HD ** -0.5
    query_full = query_block.astype(jnp.float32)
    key_full = key_block.astype(jnp.float32)
    value_full = value_block.astype(jnp.float32)
    grad_full = grad_block.astype(jnp.float32)
    positions = jnp.arange(LEN, dtype=jnp.int32)
    allowed = (positions[None, :] <= positions[:, None]) & (doc_row[None, :] == doc_row[:, None])
    scores = jnp.einsum('gid,jd->gij', query_full, key_full) * score_scale
    masked = jnp.where(allowed, scores, NEG_FILL)
    row_top = jnp.max(masked, axis=-1, keepdims=True)
    row_sum = jnp.sum(jnp.where(allowed, jnp.exp(masked - row_top), 0.0), axis=-1, keepdims=True)
    log_total = row_top + jnp.log(row_sum)
    weights = jnp.where(allowed, jnp.exp(masked - log_total), 0.0)
    weight_grad = jnp.einsum('gid,jd->gij', grad_full, value_full)
    row_delta = jnp.sum(weights * weight_grad, axis=-1, keepdims=True)
    score_grad = lax.optimization_barrier((weights * (weight_grad - row_delta) * score_scale).astype(jnp.bfloat16)).astype(jnp.float32)
    weights_low = lax.optimization_barrier(weights.astype(jnp.bfloat16)).astype(jnp.float32)
    query_part = jnp.einsum('gij,jd->gid', score_grad, key_full)
    key_part = jnp.einsum('gij,gid->jd', score_grad, query_full)
    value_part = jnp.einsum('gij,gid->jd', weights_low, grad_full)
    return query_part.astype(jnp.bfloat16), key_part, value_part


def reference(queries, key_cache, value_cache, out_grad, doc_ids, layer_input, key_proj, value_proj):
    def one_sequence(items):
        query_seq, key_seq, value_seq, grad_seq, doc_row = items
        query_heads = query_seq.reshape(LEN, KVH, GROUP, HD).transpose(1, 2, 0, 3)
        grad_heads = grad_seq.reshape(LEN, KVH, GROUP, HD).transpose(1, 2, 0, 3)
        key_heads = key_seq.reshape(LEN, KVH, HD).transpose(1, 0, 2)
        value_heads = value_seq.reshape(LEN, KVH, HD).transpose(1, 0, 2)

        def one_head(head_items):
            return head_grads(head_items[0], head_items[1], head_items[2], head_items[3], doc_row)

        query_part, key_part, value_part = lax.map(one_head, (query_heads, key_heads, value_heads, grad_heads))
        query_part = query_part.transpose(2, 0, 1, 3).reshape(LEN, QH * HD)
        key_part = key_part.transpose(1, 0, 2).reshape(LEN, KVH * HD)
        value_part = value_part.transpose(1, 0, 2).reshape(LEN, KVH * HD)
        return query_part, key_part, value_part

    query_grad, key_grad, value_grad = lax.map(one_sequence, (queries, key_cache, value_cache, out_grad, doc_ids))
    key_low = key_grad.astype(jnp.bfloat16).reshape(SEQS * LEN, KVH * HD)
    value_low = value_grad.astype(jnp.bfloat16).reshape(SEQS * LEN, KVH * HD)
    input_sum = jnp.dot(key_low, key_proj.T, preferred_element_type=jnp.float32) + jnp.dot(value_low, value_proj.T, preferred_element_type=jnp.float32)
    input_grad = input_sum.astype(jnp.bfloat16).reshape(SEQS, LEN, D)
    flat_input = layer_input.reshape(SEQS * LEN, D)
    grad_keyproj = jnp.dot(flat_input.T, key_low, preferred_element_type=jnp.float32)
    grad_valueproj = jnp.dot(flat_input.T, value_low, preferred_element_type=jnp.float32)
    return query_grad, input_grad, grad_keyproj, grad_valueproj
```

```python
import functools

import jax
import jax.numpy as jnp
from jax import lax
from jax.experimental import pallas as pl
from jax.experimental.pallas import tpu as pltpu
from jax.sharding import PartitionSpec as P

HD = 128
MASKED = -1e30
F32 = jnp.float32
BF16 = jnp.bfloat16


def dot(a, b, ca, cb):
    return lax.dot_general(a, b, (((ca,), (cb,)), ((), ())), preferred_element_type=F32)


def attention_kernel(blocks, group, *refs):
    q_ref, g_ref = refs[:2]
    k_refs, v_refs = refs[2 : 2 + blocks], refs[2 + blocks : 2 + 2 * blocks]
    docs_ref = refs[2 + 2 * blocks]
    dq_ref, own_ref = refs[3 + 2 * blocks : 5 + 2 * blocks]
    prev_refs = refs[5 + 2 * blocks :]
    rows = q_ref.shape[0]
    scale = HD**-0.5
    query_doc = docs_ref[0:1, :]
    allowed = []
    for b in range(blocks):
        key_doc = jnp.broadcast_to(docs_ref[b : b + 1, :], (HD, rows)).T[:, :1]
        same = key_doc == query_doc
        if b == 0:
            key_pos = lax.broadcasted_iota(jnp.int32, (rows, rows), 0)
            query_pos = lax.broadcasted_iota(jnp.int32, (rows, rows), 1)
            same = same & (key_pos <= query_pos)
        allowed.append(same)
    dk = [jnp.zeros((rows, HD), F32) for _ in range(blocks)]
    dv = [jnp.zeros((rows, HD), F32) for _ in range(blocks)]
    for h in range(group):
        cols = slice(h * HD, (h + 1) * HD)
        q, g = q_ref[:, cols], g_ref[:, cols]
        scores = [
            jnp.where(allowed[b], dot(k_refs[b][...], q, 1, 1) * scale, MASKED)
            for b in range(blocks)
        ]
        top = functools.reduce(jnp.maximum, [jnp.max(x, axis=0, keepdims=True) for x in scores])
        parts = [jnp.exp(x - top) for x in scores]
        total = sum(jnp.sum(x, axis=0, keepdims=True) for x in parts)
        weights = [x / total for x in parts]
        wgrads = [dot(v_refs[b][...], g, 1, 1) for b in range(blocks)]
        delta = sum(jnp.sum(w * d, axis=0, keepdims=True) for w, d in zip(weights, wgrads))
        dq = jnp.zeros((rows, HD), F32)
        for b in range(blocks):
            ds = (weights[b] * (wgrads[b] - delta) * scale).astype(BF16)
            dq += dot(ds, k_refs[b][...], 0, 0)
            dk[b] += dot(ds, q, 1, 0)
            dv[b] += dot(weights[b].astype(BF16), g, 1, 0)
        dq_ref[:, cols] = dq.astype(BF16)
    own_ref[:, :HD] = dk[0]
    own_ref[:, HD:] = dv[0]
    for b in range(1, blocks):
        prev_refs[b - 1][:, :HD] = dk[b].astype(BF16)
        prev_refs[b - 1][:, HD:] = dv[b].astype(BF16)


def attention(q, g, keys, values, docs):
    rows, width = q.shape
    blocks = len(keys)
    outs = [
        jax.ShapeDtypeStruct((rows, width), BF16),
        jax.ShapeDtypeStruct((rows, 2 * HD), F32),
    ] + [jax.ShapeDtypeStruct((rows, 2 * HD), BF16)] * (blocks - 1)
    return pl.pallas_call(
        functools.partial(attention_kernel, blocks, width // HD),
        out_shape=outs,
        name="attention",
        cost_estimate=pl.CostEstimate(
            flops=10 * rows * rows * blocks * width,
            transcendentals=rows * rows * blocks * width // HD,
            bytes_accessed=8 * rows * width,
        ),
    )(q, g, *keys, *values, docs)


def spread_kernel(chip_ref, core_ref, own_ref, other_ref, key_ref, value_ref):
    size = own_ref.shape[1]
    core = core_ref[0]
    for src, at in ((own_ref, core), (other_ref, 1 - core)):
        at = pl.ds(pl.multiple_of(at * size, 8), size)
        key_ref[at, :] = src[0, :, :HD].astype(F32)
        value_ref[at, :] = src[0, :, HD:].astype(F32)


def spread(own, other, chips, core):
    count, size, _ = own.shape
    spec = pl.BlockSpec((1, size, 2 * HD), lambda i, chip, core: (i, 0, 0))
    out = pl.BlockSpec((2 * size, HD), lambda i, chip, core: (chip[i], 0))
    shape = jax.ShapeDtypeStruct((2 * size * count, HD), F32)
    return pl.pallas_call(
        spread_kernel,
        grid_spec=pltpu.PrefetchScalarGridSpec(
            num_scalar_prefetch=2, grid=(count,), in_specs=[spec, spec], out_specs=[out, out]
        ),
        out_shape=[shape, shape],
        name="spread",
    )(chips, core, own, other)


class Plane:
    def __init__(self):
        self.dp, self.seq = lax.axis_size("dp"), lax.axis_size("seq")
        self.high = self.dp // 2
        d, self.s = lax.axis_index("dp"), lax.axis_index("seq")
        self.core, self.h = d % 2, d // 2
        self.cells = self.high * self.seq
        self.offsets = [(a, r) for a in range(self.high) for r in range(self.seq)]
        self.cell = self.h * self.seq + self.s

    def cell_at(self, a, r):
        return (self.h + a) % self.high * self.seq + (self.s + r) % self.seq

    def shift(self, x, a, r):
        pairs = []
        for h in range(self.high):
            for c in range(2):
                for s in range(self.seq):
                    to = ((h + a) % self.high * 2 + c) * self.seq + (s + r) % self.seq
                    pairs.append(((h * 2 + c) * self.seq + s, to))
        return lax.ppermute(x, ("dp", "seq"), pairs)

    def swap(self, x):
        return lax.ppermute(x, "dp", [(i, i ^ 1) for i in range(self.dp)])

    def gather(self, x):
        return jnp.stack([x] + [self.shift(x, a, r) for a, r in self.offsets[1:]])


def ring(n, r):
    return [(i, (i + r) % n) for i in range(n)]


def line_gather(x, axis):
    n = lax.axis_size(axis)
    i = lax.axis_index(axis)
    if n != 4:
        return [x] + [lax.ppermute(x, axis, ring(n, r)) for r in range(1, n)]
    two = lax.ppermute(x, axis, ring(n, 2))
    up = lax.ppermute(x, axis, [(j, j + 1) for j in range(n - 1)])
    down = lax.ppermute(x, axis, [(j + 1, j) for j in range(n - 1)])
    far = lax.ppermute(two, axis, [(n - 2, n - 1), (1, 0)])
    return [x, jnp.where(i == 0, far, up), two, jnp.where(i == n - 1, far, down)]


def shards(queries, key_cache, value_cache, out_grad, doc_ids, layer_input, key_proj, value_proj):
    plane = Plane()
    seq, heads = plane.seq, lax.axis_size("head")
    z = lax.axis_index("head")
    rows, width = queries.shape[1:]
    d_model = layer_input.shape[2]
    slab = d_model // plane.cells
    size = slab // 2
    own_slice = (plane.cell * 2 + plane.core) * size
    sub = rows // heads

    docs = doc_ids.astype(F32)
    keys, values, key_docs = [key_cache[0]], [value_cache[0]], [docs]
    for r in range(1, seq):
        pairs = [(i, i + r) for i in range(seq - r)]
        keys.append(lax.ppermute(key_cache[0], "seq", pairs))
        values.append(lax.ppermute(value_cache[0], "seq", pairs))
        key_docs.append(jnp.where(plane.s >= r, lax.ppermute(docs, "seq", pairs), -1.0))

    x = layer_input[0]
    slabs = []
    for a, r in plane.offsets:
        piece = lax.dynamic_slice_in_dim(x, plane.cell_at(a, r) * slab, slab, 1)
        slabs.append(plane.shift(piece, a, r) if (a, r) != (0, 0) else piece)
    slabs = jnp.stack(slabs).reshape(plane.cells * sub, 2, size)
    mine = lax.dynamic_index_in_dim(slabs, plane.core, 1, keepdims=False)
    theirs = lax.dynamic_index_in_dim(slabs, 1 - plane.core, 1, keepdims=False)
    x_plane = jnp.concatenate([mine, plane.swap(theirs)], axis=0)
    w_slice = jnp.concatenate(
        [lax.dynamic_slice_in_dim(w, own_slice, size, 0) for w in (key_proj, value_proj)], axis=1
    )
    w_all = line_gather(w_slice, "head")
    x_all = line_gather(x_plane, "head")

    query_grad, own_terms, *prev_terms = attention(
        queries[0], out_grad[0], keys, values, jnp.concatenate(key_docs, axis=0)
    )
    dkv = own_terms
    for r in range(1, seq):
        pairs = [(i + r, i) for i in range(seq - r)]
        dkv = dkv + lax.ppermute(prev_terms[r - 1], "seq", pairs).astype(F32)
    dkv = dkv.astype(BF16)

    dkv_own = plane.gather(dkv)
    dkv_all = jnp.concatenate([dkv_own, plane.swap(dkv_own)], axis=0)
    dkv_all = dkv_all.reshape(2 * plane.cells, heads, sub, 2 * HD)
    grad = jnp.zeros((size, 2 * HD), F32)
    for r in range(heads):
        piece = lax.dynamic_index_in_dim(dkv_all, (z - r) % heads, 1, keepdims=False)
        grad += dot(x_all[r], piece.reshape(2 * plane.cells * sub, 2 * HD), 0, 0)
    grad_own = plane.gather(grad.astype(BF16))
    grad_other = plane.swap(grad_own)
    chips = jnp.stack([plane.cell_at(-a, -r) for a, r in plane.offsets]).astype(jnp.int32)
    grad_keyproj, grad_valueproj = spread(
        grad_own, grad_other, chips, plane.core.astype(jnp.int32).reshape(1)
    )

    dkv_rows = dkv.reshape(heads, sub, 2 * HD)
    pieces = []
    for r in range(heads):
        piece = lax.dynamic_index_in_dim(dkv_rows, (z + r) % heads, 0, keepdims=False)
        pieces.append(lax.ppermute(piece, "head", ring(heads, r)) if r else piece)
    heads_own = plane.gather(jnp.concatenate(pieces, axis=1))
    heads_own = heads_own.reshape(plane.cells * sub, heads * 2 * HD)
    heads_all = jnp.concatenate([heads_own, plane.swap(heads_own)], axis=0)
    part = dot(heads_all, jnp.concatenate(w_all, axis=1), 1, 1).astype(BF16)
    part = part.reshape(2, plane.cells, sub, size)
    other = plane.swap(part[1])
    first = jnp.where(plane.core == 0, part[0], other)
    second = jnp.where(plane.core == 0, other, part[0])
    both = jnp.concatenate([first, second], axis=2)
    input_grad = jnp.zeros((sub, d_model), BF16)
    for o, (a, r) in enumerate(plane.offsets):
        piece = plane.shift(both[o], -a, -r) if o else both[o]
        input_grad = lax.dynamic_update_slice_in_dim(
            input_grad, piece, plane.cell_at(a, r) * slab, 1
        )
    return query_grad[None], input_grad[None], grad_keyproj, grad_valueproj


def solution(mesh):
    return jax.shard_map(
        shards,
        mesh=mesh,
        in_specs=(
            P("dp", "seq", "head"),
            P("dp", "seq", "head"),
            P("dp", "seq", "head"),
            P("dp", "seq", "head"),
            P("dp", "seq"),
            P("dp", ("seq", "head"), None),
            P(None, "head"),
            P(None, "head"),
        ),
        out_specs=(
            P("dp", "seq", "head"),
            P("dp", ("seq", "head"), None),
            P(None, "head"),
            P(None, "head"),
        ),
        check_vma=False,
    )
```

```python
import functools

import jax
import jax.numpy as jnp
from jax import lax
from jax.experimental import pallas as pl
from jax.experimental.pallas import tpu as pltpu
from jax.sharding import PartitionSpec as P

HD = 128
MASKED = -1e30
F32 = jnp.float32
BF16 = jnp.bfloat16
VMEM = pl.BlockSpec(memory_space=pltpu.VMEM)
SMEM = pl.BlockSpec(memory_space=pltpu.SMEM)
ANY = pl.BlockSpec(memory_space=pl.ANY)


def dot(a, b, ca, cb):
    return lax.dot_general(a, b, (((ca,), (cb,)), ((), ())), preferred_element_type=F32)


def scalars(*values):
    return jnp.stack([jnp.asarray(v, jnp.int32) for v in values])


def attention_kernel(blocks, group, at_ref, q_ref, g_ref, *refs):
    kv_refs, refs = refs[:blocks], refs[blocks:]
    dq_ref, own_ref, *prev_refs = refs
    rows = q_ref.shape[0]
    k_refs = [ref.at[:rows, :HD] for ref in kv_refs]
    v_refs = [ref.at[:rows, HD:] for ref in kv_refs]
    doc_refs = [ref.at[rows:, :rows] for ref in kv_refs]
    scale = HD**-0.5
    query_doc = doc_refs[0][...].astype(F32)
    allowed = []
    for b in range(blocks):
        key_doc = doc_refs[b][...].astype(F32)
        if b:
            key_doc = jnp.where(at_ref[3] >= b, key_doc, -1.0)
        same = jnp.broadcast_to(key_doc, (HD, rows)).T[:, :1] == query_doc
        if b == 0:
            key_pos = lax.broadcasted_iota(jnp.int32, (rows, rows), 0)
            query_pos = lax.broadcasted_iota(jnp.int32, (rows, rows), 1)
            same = same & (key_pos <= query_pos)
        allowed.append(same)
    dk = [jnp.zeros((rows, HD), F32) for _ in range(blocks)]
    dv = [jnp.zeros((rows, HD), F32) for _ in range(blocks)]
    for h in range(group):
        cols = slice(h * HD, (h + 1) * HD)
        q, g = q_ref[:, cols], g_ref[:, cols]
        scores = [
            jnp.where(allowed[b], dot(k_refs[b][...], q, 1, 1) * scale, MASKED)
            for b in range(blocks)
        ]
        top = functools.reduce(jnp.maximum, [jnp.max(x, axis=0, keepdims=True) for x in scores])
        parts = [jnp.exp(x - top) for x in scores]
        total = sum(jnp.sum(x, axis=0, keepdims=True) for x in parts)
        inverse = 1.0 / total
        weights = [x * inverse for x in parts]
        wgrads = [dot(v_refs[b][...], g, 1, 1) for b in range(blocks)]
        delta = sum(jnp.sum(w * d, axis=0, keepdims=True) for w, d in zip(weights, wgrads))
        dq = jnp.zeros((rows, HD), F32)
        for b in range(blocks):
            ds = (weights[b] * (wgrads[b] - delta) * scale).astype(BF16)
            dq += dot(ds, k_refs[b][...], 0, 0)
            dk[b] += dot(ds, q, 1, 0)
            dv[b] += dot(weights[b].astype(BF16), g, 1, 0)
        dq_ref[:, cols] = dq.astype(BF16)
    own_ref[:, :HD] = dk[0]
    own_ref[:, HD:] = dv[0]
    for b in range(1, blocks):
        prev_refs[b - 1][:, :HD] = dk[b].astype(BF16)
        prev_refs[b - 1][:, HD:] = dv[b].astype(BF16)


def attention(at, q, g, packs):
    rows, width = q.shape
    blocks = len(packs)
    outs = [
        jax.ShapeDtypeStruct((rows, width), BF16),
        jax.ShapeDtypeStruct((rows, 2 * HD), F32),
    ] + [jax.ShapeDtypeStruct((rows, 2 * HD), BF16)] * (blocks - 1)
    return pl.pallas_call(
        functools.partial(attention_kernel, blocks, width // HD),
        out_shape=outs,
        in_specs=[SMEM] + [VMEM] * (2 + blocks),
        name="attention",
        cost_estimate=pl.CostEstimate(
            flops=10 * rows * rows * blocks * width,
            transcendentals=rows * rows * blocks * width // HD,
            bytes_accessed=8 * rows * width,
        ),
    )(at, q, g, *packs)


def grads_kernel(slots, sub, fars, at_ref, *refs):
    count = len(slots)
    x_refs, refs = refs[: count + fars], refs[count + fars :]
    own_ref, other_ref, *add_refs, out_ref = refs
    z = at_ref[0]
    half = own_ref.shape[0] * sub
    total = jnp.zeros(out_ref.shape, F32)
    for ref in add_refs:
        total += ref[...]
    for i, r in enumerate(slots):
        x = x_refs[i][...]
        if fars and i == count - 1:
            x = jnp.where((z == 0) | (z == r), x_refs[count][...], x)
        start = pl.multiple_of((z ^ r) * sub, sub)
        pieces = [
            ref[:, pl.ds(start, sub), :].reshape(half, out_ref.shape[1])
            for ref in (own_ref, other_ref)
        ]
        total += dot(x, jnp.concatenate(pieces, axis=0), 0, 0)
    out_ref[...] = total.astype(out_ref.dtype)


def grads(at, xs, slots, own, other, adds, dtype):
    sub = xs[0].shape[0] // (2 * own.shape[0])
    size, width = xs[0].shape[1], own.shape[2]
    return pl.pallas_call(
        functools.partial(grads_kernel, tuple(slots), sub, len(xs) - len(slots)),
        out_shape=jax.ShapeDtypeStruct((size, width), dtype),
        in_specs=[SMEM] + [VMEM] * (len(xs) + 2 + len(adds)),
        cost_estimate=pl.CostEstimate(
            flops=2 * len(xs) * xs[0].size * width, transcendentals=0, bytes_accessed=2 * xs[0].size
        ),
    )(at, *xs, own, other, *adds)


def input_kernel(heads, own_ref, other_ref, *refs):
    row_refs, out_refs = refs[:heads], refs[heads:]
    size, sub = own_ref.shape[1], out_refs[0].shape[0]
    for j, w_ref in enumerate((own_ref, other_ref)):
        part = sum(dot(row_refs[r][...], w_ref[r], 1, 1) for r in range(heads))
        for o, out_ref in enumerate(out_refs):
            out_ref[:, j * size : (j + 1) * size] = part[o * sub : (o + 1) * sub].astype(BF16)


def input_parts(w_own, w_other, rows, cells):
    heads, size, sub = len(rows), w_own.shape[1], rows[0].shape[0] // cells
    return pl.pallas_call(
        functools.partial(input_kernel, heads),
        out_shape=[jax.ShapeDtypeStruct((sub, 2 * size), BF16)] * cells,
        in_specs=[VMEM] * (heads + 2),
        name="input_grads",
        cost_estimate=pl.CostEstimate(
            flops=4 * cells * sub * w_own.size, transcendentals=0, bytes_accessed=4 * w_own.size
        ),
    )(w_own, w_other, *rows)


def place_kernel(cells, at_ref, *refs):
    size = refs[0].shape[1] // 2
    out_ref = refs[cells]
    for o in range(cells):
        base = (at_ref[1] ^ o) * 2
        for j, core in ((0, at_ref[2]), (1, 1 - at_ref[2])):
            start = (base + core) * size
            if size % HD == 0:
                start = pl.multiple_of(start, HD)
            out_ref[:, pl.ds(start, size)] = refs[o][:, j * size : (j + 1) * size]


def place(at, pieces):
    cells, (sub, slab) = len(pieces), pieces[0].shape
    if slab % (2 * HD):
        out = jnp.zeros((sub, slab * cells), BF16)
        for o, piece in enumerate(pieces):
            for j, half in enumerate(jnp.split(piece, 2, axis=1)):
                start = ((at[1] ^ o) * 2 + (at[2] ^ j)) * (slab // 2)
                out = lax.dynamic_update_slice_in_dim(out, half, start, 1)
        return out
    return pl.pallas_call(
        functools.partial(place_kernel, cells),
        out_shape=jax.ShapeDtypeStruct((sub, slab * cells), BF16),
        in_specs=[SMEM] + [VMEM] * cells,
        name="place",
    )(at, *pieces)


def spread_kernel(places, at_ref, *refs):
    pieces, (key_ref, value_ref, *bufs, sems) = refs[: len(places)], refs[-5:]
    size = pieces[0].shape[0]
    waits = []
    for i, ((o, flip), piece) in enumerate(zip(places, pieces)):
        base = pl.multiple_of(((at_ref[1] ^ o) * 2 + (at_ref[2] ^ flip)) * size, 8)
        for n, (out_ref, buf) in enumerate(zip((key_ref, value_ref), bufs)):
            buf[i] = piece[:, n * HD : (n + 1) * HD].astype(F32)
            copy = pltpu.make_async_copy(
                buf.at[i], out_ref.at[pl.ds(base, size), :], sems.at[n, i]
            )
            copy.start()
            waits.append(copy)
    for copy in waits:
        copy.wait()


def spread(at, total, items, outs=()):
    count, size = len(items), items[0][2].shape[0]
    shape = jax.ShapeDtypeStruct((total, HD), F32)
    buf = pltpu.VMEM((count, size, HD), F32)
    return pl.pallas_call(
        functools.partial(spread_kernel, tuple(item[:2] for item in items)),
        out_shape=[shape, shape],
        in_specs=[SMEM] + [VMEM] * count + [ANY] * len(outs),
        out_specs=[ANY, ANY],
        scratch_shapes=[buf, buf, pltpu.SemaphoreType.DMA((2, count))],
        input_output_aliases={1 + count + n: n for n in range(len(outs))},
    )(at, *[item[2] for item in items], *outs)


def swap_pairs(n, m):
    return [(i, i ^ m) for i in range(n)]


def far_first(count):
    return sorted(range(1, count), key=lambda m: (-bin(m).count("1"), -m))


def line_exchange(x):
    n = lax.axis_size("head")
    slots = {0: x}
    for r in head_offsets(n):
        pairs = swap_pairs(n, r)
        if n == 4 and r == 3:
            pairs = [(0, 0), (1, 2), (2, 1), (3, 3)]
        slots[r] = lax.ppermute(x, "head", pairs)
    out = [slots[r] for r in range(n)]
    if n == 4:
        out.append(lax.ppermute(slots[2], "head", swap_pairs(n, 1)))
    return out


def head_offsets(n):
    return [2, 1, 3] if n == 4 else list(range(1, n))


def shards(queries, key_cache, value_cache, out_grad, doc_ids, layer_input, key_proj, value_proj):
    dp, seq, heads = (lax.axis_size(a) for a in ("dp", "seq", "head"))
    d, s, z = (lax.axis_index(a) for a in ("dp", "seq", "head"))
    plane, cells = dp * seq, dp // 2 * seq
    core, cell = d % 2, d // 2 * seq + s
    rows, _ = queries.shape[1:]
    d_model = layer_input.shape[2]
    size = d_model // plane
    sub = rows // heads
    both = ("dp", "seq")

    def member(o, c):
        return (o // seq * 2 + c) * seq + o % seq

    def cell_gather(x):
        got = {0: x}
        for o in far_first(cells):
            got[o] = lax.ppermute(x, both, swap_pairs(plane, member(o, 0)))
        return [got[o] for o in range(cells)]

    def core_swap(x):
        return lax.ppermute(x, "dp", swap_pairs(dp, 1))

    pack = jnp.concatenate([key_cache[0], value_cache[0]], axis=1)
    lanes = max(rows, 2 * HD)
    pack = jnp.concatenate(
        [
            jnp.pad(pack, ((0, 0), (0, lanes - 2 * HD))),
            jnp.pad(doc_ids.astype(BF16), ((0, 0), (0, lanes - rows))),
        ],
        axis=0,
    )
    packs = [pack]
    for r in range(1, seq):
        pairs = [(i, (i + r) % seq) for i in range(seq)]
        packs.append(lax.ppermute(pack, "seq", pairs))

    x = layer_input[0]
    got = []
    for o in range(cells):
        piece = lax.dynamic_slice_in_dim(x, (cell ^ o) * 2 * size, 2 * size, 1)
        if o:
            piece = lax.ppermute(piece, both, swap_pairs(plane, member(o, 0)))
        got.append(piece)
    got = jnp.concatenate(got, axis=0)
    mine = lax.dynamic_slice_in_dim(got, core * size, size, 1)
    theirs = lax.dynamic_slice_in_dim(got, (1 - core) * size, size, 1)
    x_plane = jnp.concatenate([mine, core_swap(theirs)], axis=0)

    own_slice = (cell * 2 + core) * size
    w_slice = jnp.concatenate(
        [lax.dynamic_slice_in_dim(w, own_slice, size, 0) for w in (key_proj, value_proj)], axis=1
    )
    w_slots = line_exchange(w_slice)
    x_slots = line_exchange(x_plane)
    at = scalars(z, cell, core, s)

    query_grad, own_terms, *prev_terms = attention(at, queries[0], out_grad[0], packs)
    dkv = own_terms
    for r in range(1, seq):
        pairs = [(i, (i - r) % seq) for i in range(seq)]
        dkv = dkv + lax.ppermute(prev_terms[r - 1], "seq", pairs).astype(F32)
    dkv = dkv.astype(BF16)

    dkv_own = jnp.stack(cell_gather(dkv))
    dkv_other = core_swap(dkv_own)
    head_rows = []
    for r in range(heads):
        piece = lax.dynamic_slice_in_dim(dkv_own, (z ^ r) * sub, sub, 1)
        piece = piece.reshape(cells * sub, 2 * HD)
        head_rows.append(lax.ppermute(piece, "head", swap_pairs(heads, r)) if r else piece)

    slots = list(range(heads))
    part = grads(at, x_slots[: heads - 1], slots[:-1], dkv_own, dkv_other, [], F32)
    grad = grads(at, x_slots[heads - 1 :], slots[-1:], dkv_own, dkv_other, [part], BF16)
    grad_own = cell_gather(grad)
    items = [(o, 0, g) for o, g in enumerate(grad_own)]
    items += [(o, 1, core_swap(g)) for o, g in enumerate(grad_own)]
    outs = spread(at, d_model, [i for i in items if i[0] == 0])
    grad_keyproj, grad_valueproj = spread(at, d_model, [i for i in items if i[0]], outs)

    if len(w_slots) > heads:
        outer = (z == 0) | (z == heads - 1)
        w_slots = w_slots[: heads - 1] + [jnp.where(outer, w_slots[heads], w_slots[heads - 1])]
    w_own = jnp.stack(w_slots)
    parts = list(input_parts(w_own, core_swap(w_own), head_rows, cells))
    for o in far_first(cells):
        parts[o] = lax.ppermute(parts[o], both, swap_pairs(plane, member(o, 0)))
    input_grad = place(at, parts)
    return query_grad[None], input_grad[None], grad_keyproj, grad_valueproj


def solution(mesh):
    return jax.shard_map(
        shards,
        mesh=mesh,
        in_specs=(
            P("dp", "seq", "head"),
            P("dp", "seq", "head"),
            P("dp", "seq", "head"),
            P("dp", "seq", "head"),
            P("dp", "seq"),
            P("dp", ("seq", "head"), None),
            P(None, "head"),
            P(None, "head"),
        ),
        out_specs=(
            P("dp", "seq", "head"),
            P("dp", ("seq", "head"), None),
            P(None, "head"),
            P(None, "head"),
        ),
        check_vma=False,
    )
```

```python
import functools

import jax
import jax.numpy as jnp
from jax import lax
from jax.experimental import pallas as pl
from jax.experimental.pallas import tpu as pltpu
from jax.sharding import PartitionSpec as P

HD = 128
MASKED = -1e30
F32 = jnp.float32
BF16 = jnp.bfloat16
VMEM = pl.BlockSpec(memory_space=pltpu.VMEM)
SMEM = pl.BlockSpec(memory_space=pltpu.SMEM)
ANY = pl.BlockSpec(memory_space=pl.ANY)


def dot(a, b, ca, cb):
    return lax.dot_general(a, b, (((ca,), (cb,)), ((), ())), preferred_element_type=F32)


def scalars(*values):
    return jnp.stack([jnp.asarray(v, jnp.int32) for v in values])


def attention_kernel(blocks, group, at_ref, q_ref, g_ref, *refs):
    kv_refs, refs = refs[:blocks], refs[blocks:]
    dq_ref, own_ref, *prev_refs = refs
    rows = q_ref.shape[0]
    k_refs = [ref.at[:rows, :HD] for ref in kv_refs]
    v_refs = [ref.at[:rows, HD:] for ref in kv_refs]
    doc_refs = [ref.at[rows:, :rows] for ref in kv_refs]
    scale = HD**-0.5
    query_doc = doc_refs[0][...].astype(F32)
    allowed = []
    for b in range(blocks):
        key_doc = doc_refs[b][...].astype(F32)
        if b:
            key_doc = jnp.where(at_ref[3] >= b, key_doc, -1.0)
        same = jnp.broadcast_to(key_doc, (HD, rows)).T[:, :1] == query_doc
        if b == 0:
            key_pos = lax.broadcasted_iota(jnp.int32, (rows, rows), 0)
            query_pos = lax.broadcasted_iota(jnp.int32, (rows, rows), 1)
            same = same & (key_pos <= query_pos)
        allowed.append(same)
    dk = [jnp.zeros((rows, HD), F32) for _ in range(blocks)]
    dv = [jnp.zeros((rows, HD), F32) for _ in range(blocks)]
    for h in range(group):
        cols = slice(h * HD, (h + 1) * HD)
        q, g = q_ref[:, cols], g_ref[:, cols]
        scores = [
            jnp.where(allowed[b], dot(k_refs[b][...], q, 1, 1) * scale, MASKED)
            for b in range(blocks)
        ]
        top = functools.reduce(jnp.maximum, [jnp.max(x, axis=0, keepdims=True) for x in scores])
        parts = [jnp.exp(x - top) for x in scores]
        total = sum(jnp.sum(x, axis=0, keepdims=True) for x in parts)
        inverse = 1.0 / total
        weights = [x * inverse for x in parts]
        wgrads = [dot(v_refs[b][...], g, 1, 1) for b in range(blocks)]
        delta = sum(jnp.sum(w * d, axis=0, keepdims=True) for w, d in zip(weights, wgrads))
        dq = jnp.zeros((rows, HD), F32)
        for b in range(blocks):
            ds = (weights[b] * (wgrads[b] - delta) * scale).astype(BF16)
            dq += dot(ds, k_refs[b][...], 0, 0)
            dk[b] += dot(ds, q, 1, 0)
            dv[b] += dot(weights[b].astype(BF16), g, 1, 0)
        dq_ref[:, cols] = dq.astype(BF16)
    own_ref[:, :HD] = dk[0]
    own_ref[:, HD:] = dv[0]
    for b in range(1, blocks):
        prev_refs[b - 1][:, :HD] = dk[b].astype(BF16)
        prev_refs[b - 1][:, HD:] = dv[b].astype(BF16)


def attention(at, q, g, packs):
    rows, width = q.shape
    blocks = len(packs)
    outs = [
        jax.ShapeDtypeStruct((rows, width), BF16),
        jax.ShapeDtypeStruct((rows, 2 * HD), F32),
    ] + [jax.ShapeDtypeStruct((rows, 2 * HD), BF16)] * (blocks - 1)
    return pl.pallas_call(
        functools.partial(attention_kernel, blocks, width // HD),
        out_shape=outs,
        in_specs=[SMEM] + [VMEM] * (2 + blocks),
        name="attention",
        cost_estimate=pl.CostEstimate(
            flops=10 * rows * rows * blocks * width,
            transcendentals=rows * rows * blocks * width // HD,
            bytes_accessed=8 * rows * width,
        ),
    )(at, q, g, *packs)


def input_kernel(heads, own_ref, other_ref, *refs):
    row_refs, out_refs = refs[:heads], refs[heads:]
    size, sub = own_ref.shape[1], out_refs[0].shape[0]
    for j, w_ref in enumerate((own_ref, other_ref)):
        part = sum(dot(row_refs[r][...], w_ref[r], 1, 1) for r in range(heads))
        for o, out_ref in enumerate(out_refs):
            out_ref[:, j * size : (j + 1) * size] = part[o * sub : (o + 1) * sub].astype(BF16)


def input_parts(w_own, w_other, rows, cells):
    heads, size, sub = len(rows), w_own.shape[1], rows[0].shape[0] // cells
    return pl.pallas_call(
        functools.partial(input_kernel, heads),
        out_shape=[jax.ShapeDtypeStruct((sub, 2 * size), BF16)] * cells,
        in_specs=[VMEM] * (heads + 2),
        name="input_grads",
        cost_estimate=pl.CostEstimate(
            flops=4 * cells * sub * w_own.size, transcendentals=0, bytes_accessed=4 * w_own.size
        ),
    )(w_own, w_other, *rows)


def place(at, pieces):
    cells, (sub, slab) = len(pieces), pieces[0].shape
    out = jnp.zeros((sub, slab * cells), BF16)
    for o, piece in enumerate(pieces):
        for j, half in enumerate(jnp.split(piece, 2, axis=1)):
            start = ((at[1] ^ o) * 2 + (at[2] ^ j)) * (slab // 2)
            out = lax.dynamic_update_slice_in_dim(out, half, start, 1)
    return out


def spread_kernel(places, parts, at_ref, *refs):
    pieces, refs = refs[: len(places)], refs[len(places) :]
    part_refs, (key_ref, value_ref, *placed, key_buf, value_buf, sems) = refs[:parts], refs[-6:]
    if not parts:
        key_ref, value_ref = refs[-5:-3]
    size = pieces[0].shape[0]
    waits = []
    for i, ((o, flip), piece) in enumerate(zip(places, pieces)):
        base = pl.multiple_of(((at_ref[1] ^ o) * 2 + (at_ref[2] ^ flip)) * size, 8)
        for n, (out_ref, buf) in enumerate(((key_ref, key_buf), (value_ref, value_buf))):
            buf[i] = piece[:, n * HD : (n + 1) * HD].astype(F32)
            copy = pltpu.make_async_copy(
                buf.at[i], out_ref.at[pl.ds(base, size), :], sems.at[n, i]
            )
            copy.start()
            waits.append(copy)
    for o, ref in enumerate(part_refs):
        for j in range(2):
            start = pl.multiple_of(((at_ref[1] ^ o) * 2 + (at_ref[2] ^ j)) * size, HD)
            placed[0][:, pl.ds(start, size)] = ref[:, j * size : (j + 1) * size]
    for copy in waits:
        copy.wait()


def spread(at, total, items, outs=(), parts=()):
    count, size = len(items), items[0][2].shape[0]
    shapes = [jax.ShapeDtypeStruct((total, HD), F32)] * 2
    buf = pltpu.VMEM((count, size, HD), F32)
    specs = [ANY, ANY]
    if parts:
        shapes.append(jax.ShapeDtypeStruct((parts[0].shape[0], total), BF16))
        specs.append(VMEM)
    first = 1 + count + len(parts)
    return pl.pallas_call(
        functools.partial(spread_kernel, tuple(item[:2] for item in items), len(parts)),
        out_shape=shapes,
        in_specs=[SMEM] + [VMEM] * (count + len(parts)) + [ANY] * len(outs),
        out_specs=specs,
        scratch_shapes=[buf, buf, pltpu.SemaphoreType.DMA((2, count))],
        input_output_aliases={first + n: n for n in range(len(outs))},
    )(at, *[item[2] for item in items], *parts, *outs)


def swap_pairs(n, m):
    return [(i, i ^ m) for i in range(n)]


def far_first(count):
    return sorted(range(1, count), key=lambda m: (-bin(m).count("1"), -m))


def line_exchange(x):
    n = lax.axis_size("head")
    slots = {0: x}
    for r in head_offsets(n):
        pairs = swap_pairs(n, r)
        if n == 4 and r == 3:
            pairs = [(0, 0), (1, 2), (2, 1), (3, 3)]
        slots[r] = lax.ppermute(x, "head", pairs)
    out = [slots[r] for r in range(n)]
    if n == 4:
        out.append(lax.ppermute(slots[2], "head", swap_pairs(n, 1)))
    return out


def head_offsets(n):
    return [2, 1, 3] if n == 4 else list(range(1, n))


def shards(queries, key_cache, value_cache, out_grad, doc_ids, layer_input, key_proj, value_proj):
    dp, seq, heads = (lax.axis_size(a) for a in ("dp", "seq", "head"))
    d, s, z = (lax.axis_index(a) for a in ("dp", "seq", "head"))
    plane, cells = dp * seq, dp // 2 * seq
    core, cell = d % 2, d // 2 * seq + s
    rows, _ = queries.shape[1:]
    d_model = layer_input.shape[2]
    size = d_model // plane
    sub = rows // heads
    both = ("dp", "seq")

    def member(o, c):
        return (o // seq * 2 + c) * seq + o % seq

    def cell_gather(x):
        got = {0: x}
        for o in far_first(cells):
            got[o] = lax.ppermute(x, both, swap_pairs(plane, member(o, 0)))
        return [got[o] for o in range(cells)]

    def core_swap(x):
        return lax.ppermute(x, "dp", swap_pairs(dp, 1))

    pack = jnp.concatenate([key_cache[0], value_cache[0]], axis=1)
    lanes = max(rows, 2 * HD)
    pack = jnp.concatenate(
        [
            jnp.pad(pack, ((0, 0), (0, lanes - 2 * HD))),
            jnp.pad(doc_ids.astype(BF16), ((0, 0), (0, lanes - rows))),
        ],
        axis=0,
    )
    packs = [pack]
    for r in range(1, seq):
        pairs = [(i, (i + r) % seq) for i in range(seq)]
        packs.append(lax.ppermute(pack, "seq", pairs))

    x = layer_input[0]
    got = []
    for o in range(cells):
        piece = lax.dynamic_slice_in_dim(x, (cell ^ o) * 2 * size, 2 * size, 1)
        if o:
            piece = lax.ppermute(piece, both, swap_pairs(plane, member(o, 0)))
        got.append(piece)
    got = jnp.concatenate(got, axis=0)
    mine = lax.dynamic_slice_in_dim(got, core * size, size, 1)
    theirs = lax.dynamic_slice_in_dim(got, (1 - core) * size, size, 1)
    x_plane = jnp.concatenate([mine, core_swap(theirs)], axis=0)

    own_slice = (cell * 2 + core) * size
    w_slice = jnp.concatenate(
        [lax.dynamic_slice_in_dim(w, own_slice, size, 0) for w in (key_proj, value_proj)], axis=1
    )
    w_slots = line_exchange(w_slice)
    x_slots = line_exchange(x_plane)
    at = scalars(z, cell, core, s)

    query_grad, own_terms, *prev_terms = attention(at, queries[0], out_grad[0], packs)
    terms = []
    for r in range(1, seq):
        pairs = [(i, (i - r) % seq) for i in range(seq)]
        terms.append(lax.ppermute(prev_terms[r - 1], "seq", pairs))
    dkv = sum([t.astype(F32) for t in terms], own_terms).astype(BF16)

    dkv_own = jnp.stack(cell_gather(dkv))
    dkv_other = core_swap(dkv_own)
    head_rows, both_rows = [], []
    for r in range(heads):
        own, other = (
            lax.dynamic_slice_in_dim(t, (z ^ r) * sub, sub, 1).reshape(cells * sub, 2 * HD)
            for t in (dkv_own, dkv_other)
        )
        head_rows.append(lax.ppermute(own, "head", swap_pairs(heads, r)) if r else own)
        both_rows.append(jnp.concatenate([own, other], axis=0))
    outer = (z == 0) | (z == heads - 1)

    if len(x_slots) > heads:
        x_slots = x_slots[: heads - 1] + [jnp.where(outer, x_slots[heads], x_slots[heads - 1])]
    grad = sum(dot(x_slots[r], both_rows[r], 0, 0) for r in range(heads)).astype(BF16)
    grad_own = cell_gather(grad)
    items = [(o, 0, g) for o, g in enumerate(grad_own)]
    items += [(o, 1, core_swap(g)) for o, g in enumerate(grad_own)]
    outs = spread(at, d_model, [i for i in items if i[0] == 0])

    if len(w_slots) > heads:
        w_slots = w_slots[: heads - 1] + [jnp.where(outer, w_slots[heads], w_slots[heads - 1])]
    w_own = jnp.stack(w_slots)
    parts = list(input_parts(w_own, core_swap(w_own), head_rows, cells))
    for o in far_first(cells):
        parts[o] = lax.ppermute(parts[o], both, swap_pairs(plane, member(o, 0)))
    rest = [i for i in items if i[0]]
    if size % HD:
        grad_keyproj, grad_valueproj = spread(at, d_model, rest, outs)
        input_grad = place(at, parts)
    else:
        grad_keyproj, grad_valueproj, input_grad = spread(at, d_model, rest, outs, parts)
    return query_grad[None], input_grad[None], grad_keyproj, grad_valueproj


def solution(mesh):
    return jax.shard_map(
        shards,
        mesh=mesh,
        in_specs=(
            P("dp", "seq", "head"),
            P("dp", "seq", "head"),
            P("dp", "seq", "head"),
            P("dp", "seq", "head"),
            P("dp", "seq"),
            P("dp", ("seq", "head"), None),
            P(None, "head"),
            P(None, "head"),
        ),
        out_specs=(
            P("dp", "seq", "head"),
            P("dp", ("seq", "head"), None),
            P(None, "head"),
            P(None, "head"),
        ),
        check_vma=False,
    )
```

```python
import functools

import jax
import jax.numpy as jnp
from jax import lax
from jax.experimental import pallas as pl
from jax.experimental.pallas import tpu as pltpu
from jax.sharding import PartitionSpec as P

HD = 128
MASKED = -1e30
F32 = jnp.float32
BF16 = jnp.bfloat16
VMEM = pl.BlockSpec(memory_space=pltpu.VMEM)
SMEM = pl.BlockSpec(memory_space=pltpu.SMEM)
ANY = pl.BlockSpec(memory_space=pl.ANY)


def dot(a, b, ca, cb):
    return lax.dot_general(a, b, (((ca,), (cb,)), ((), ())), preferred_element_type=F32)


def scalars(*values):
    return jnp.stack([jnp.asarray(v, jnp.int32) for v in values])


def attention_kernel(blocks, group, at_ref, q_ref, g_ref, *refs):
    kv_refs, refs = refs[:blocks], refs[blocks:]
    dq_ref, own_ref, *prev_refs = refs
    rows = q_ref.shape[0]
    k_refs = [ref.at[:rows, :HD] for ref in kv_refs]
    v_refs = [ref.at[:rows, HD:] for ref in kv_refs]
    doc_refs = [ref.at[rows:, :rows] for ref in kv_refs]
    scale = HD**-0.5
    query_doc = doc_refs[0][...].astype(F32)
    allowed = []
    for b in range(blocks):
        key_doc = doc_refs[b][...].astype(F32)
        if b:
            key_doc = jnp.where(at_ref[3] >= b, key_doc, -1.0)
        same = jnp.broadcast_to(key_doc, (HD, rows)).T[:, :1] == query_doc
        if b == 0:
            key_pos = lax.broadcasted_iota(jnp.int32, (rows, rows), 0)
            query_pos = lax.broadcasted_iota(jnp.int32, (rows, rows), 1)
            same = same & (key_pos <= query_pos)
        allowed.append(same)
    dk = [jnp.zeros((rows, HD), F32) for _ in range(blocks)]
    dv = [jnp.zeros((rows, HD), F32) for _ in range(blocks)]
    for h in range(group):
        cols = slice(h * HD, (h + 1) * HD)
        q, g = q_ref[:, cols], g_ref[:, cols]
        scores = [
            jnp.where(allowed[b], dot(k_refs[b][...], q, 1, 1) * scale, MASKED)
            for b in range(blocks)
        ]
        top = functools.reduce(jnp.maximum, [jnp.max(x, axis=0, keepdims=True) for x in scores])
        parts = [jnp.exp(x - top) for x in scores]
        total = sum(jnp.sum(x, axis=0, keepdims=True) for x in parts)
        inverse = 1.0 / total
        weights = [x * inverse for x in parts]
        wgrads = [dot(v_refs[b][...], g, 1, 1) for b in range(blocks)]
        delta = sum(jnp.sum(w * d, axis=0, keepdims=True) for w, d in zip(weights, wgrads))
        dq = jnp.zeros((rows, HD), F32)
        for b in range(blocks):
            ds = (weights[b] * (wgrads[b] - delta) * scale).astype(BF16)
            dq += dot(ds, k_refs[b][...], 0, 0)
            dk[b] += dot(ds, q, 1, 0)
            dv[b] += dot(weights[b].astype(BF16), g, 1, 0)
        dq_ref[:, cols] = dq.astype(BF16)
    own_ref[:, :HD] = dk[0]
    own_ref[:, HD:] = dv[0]
    for b in range(1, blocks):
        prev_refs[b - 1][:, :HD] = dk[b].astype(BF16)
        prev_refs[b - 1][:, HD:] = dv[b].astype(BF16)


def attention(at, q, g, packs):
    rows, width = q.shape
    blocks = len(packs)
    outs = [
        jax.ShapeDtypeStruct((rows, width), BF16),
        jax.ShapeDtypeStruct((rows, 2 * HD), F32),
    ] + [jax.ShapeDtypeStruct((rows, 2 * HD), BF16)] * (blocks - 1)
    return pl.pallas_call(
        functools.partial(attention_kernel, blocks, width // HD),
        out_shape=outs,
        in_specs=[SMEM] + [VMEM] * (2 + blocks),
        name="attention",
        cost_estimate=pl.CostEstimate(
            flops=10 * rows * rows * blocks * width,
            transcendentals=rows * rows * blocks * width // HD,
            bytes_accessed=8 * rows * width,
        ),
    )(at, q, g, *packs)


def input_kernel(cells, own_ref, other_ref, *refs):
    row_refs, out_refs = refs[:cells], refs[cells:]
    sub = row_refs[0].shape[0]
    heads, size, width = own_ref.shape
    rows = jnp.concatenate([ref[...] for ref in row_refs], axis=0)
    for j, w_ref in enumerate((own_ref, other_ref)):
        part = sum(
            dot(rows[:, r * width : (r + 1) * width], w_ref[r], 1, 1) for r in range(heads)
        )
        for o, out_ref in enumerate(out_refs):
            out_ref[:, j * size : (j + 1) * size] = part[o * sub : (o + 1) * sub].astype(BF16)


def input_parts(w_own, w_other, rows):
    cells, sub, size = len(rows), rows[0].shape[0], w_own.shape[1]
    return pl.pallas_call(
        functools.partial(input_kernel, cells),
        out_shape=[jax.ShapeDtypeStruct((sub, 2 * size), BF16)] * cells,
        in_specs=[VMEM] * (cells + 2),
        name="input_grads",
        cost_estimate=pl.CostEstimate(
            flops=4 * cells * sub * w_own.size, transcendentals=0, bytes_accessed=4 * w_own.size
        ),
    )(w_own, w_other, *rows)


def place(at, pieces):
    cells, (sub, slab) = len(pieces), pieces[0].shape
    out = jnp.zeros((sub, slab * cells), BF16)
    for o, piece in enumerate(pieces):
        for j, half in enumerate(jnp.split(piece, 2, axis=1)):
            start = ((at[1] ^ o) * 2 + (at[2] ^ j)) * (slab // 2)
            out = lax.dynamic_update_slice_in_dim(out, half, start, 1)
    return out


def spread_kernel(places, parts, at_ref, *refs):
    pieces, refs = refs[: len(places)], refs[len(places) :]
    part_refs, (key_ref, value_ref, *placed, key_buf, value_buf, sems) = refs[:parts], refs[-6:]
    if not parts:
        key_ref, value_ref = refs[-5:-3]
    size = pieces[0].shape[0]
    waits = []
    for i, ((o, flip), piece) in enumerate(zip(places, pieces)):
        base = pl.multiple_of(((at_ref[1] ^ o) * 2 + (at_ref[2] ^ flip)) * size, 8)
        for n, (out_ref, buf) in enumerate(((key_ref, key_buf), (value_ref, value_buf))):
            buf[i] = piece[:, n * HD : (n + 1) * HD].astype(F32)
            copy = pltpu.make_async_copy(
                buf.at[i], out_ref.at[pl.ds(base, size), :], sems.at[n, i]
            )
            copy.start()
            waits.append(copy)
    for o, ref in enumerate(part_refs):
        for j in range(2):
            start = pl.multiple_of(((at_ref[1] ^ o) * 2 + (at_ref[2] ^ j)) * size, HD)
            placed[0][:, pl.ds(start, size)] = ref[:, j * size : (j + 1) * size]
    for copy in waits:
        copy.wait()


def spread(at, total, items, outs=(), parts=()):
    count, size = len(items), items[0][2].shape[0]
    shapes = [jax.ShapeDtypeStruct((total, HD), F32)] * 2
    buf = pltpu.VMEM((count, size, HD), F32)
    specs = [ANY, ANY]
    if parts:
        shapes.append(jax.ShapeDtypeStruct((parts[0].shape[0], total), BF16))
        specs.append(VMEM)
    first = 1 + count + len(parts)
    return pl.pallas_call(
        functools.partial(spread_kernel, tuple(item[:2] for item in items), len(parts)),
        out_shape=shapes,
        in_specs=[SMEM] + [VMEM] * (count + len(parts)) + [ANY] * len(outs),
        out_specs=specs,
        scratch_shapes=[buf, buf, pltpu.SemaphoreType.DMA((2, count))],
        input_output_aliases={first + n: n for n in range(len(outs))},
    )(at, *[item[2] for item in items], *parts, *outs)


def swap_pairs(n, m):
    return [(i, i ^ m) for i in range(n)]


def far_first(count):
    return sorted(range(1, count), key=lambda m: (-bin(m).count("1"), -m))


def line_exchange(x):
    n = lax.axis_size("head")
    slots = {0: x}
    for r in head_offsets(n):
        pairs = swap_pairs(n, r)
        if n == 4 and r == 3:
            pairs = [(0, 0), (1, 2), (2, 1), (3, 3)]
        slots[r] = lax.ppermute(x, "head", pairs)
    out = [slots[r] for r in range(n)]
    if n == 4:
        out.append(lax.ppermute(slots[2], "head", swap_pairs(n, 1)))
    return out


def head_offsets(n):
    return [2, 1, 3] if n == 4 else list(range(1, n))


def shards(queries, key_cache, value_cache, out_grad, doc_ids, layer_input, key_proj, value_proj):
    dp, seq, heads = (lax.axis_size(a) for a in ("dp", "seq", "head"))
    d, s, z = (lax.axis_index(a) for a in ("dp", "seq", "head"))
    plane, cells = dp * seq, dp // 2 * seq
    core, cell = d % 2, d // 2 * seq + s
    rows, _ = queries.shape[1:]
    d_model = layer_input.shape[2]
    size = d_model // plane
    sub = rows // heads
    both = ("dp", "seq")

    def member(o, c):
        return (o // seq * 2 + c) * seq + o % seq

    def cell_gather(x):
        got = {0: x}
        for o in far_first(cells):
            got[o] = lax.ppermute(x, both, swap_pairs(plane, member(o, 0)))
        return [got[o] for o in range(cells)]

    def core_swap(x):
        return lax.ppermute(x, "dp", swap_pairs(dp, 1))

    pack = jnp.concatenate([key_cache[0], value_cache[0]], axis=1)
    lanes = max(rows, 2 * HD)
    pack = jnp.concatenate(
        [
            jnp.pad(pack, ((0, 0), (0, lanes - 2 * HD))),
            jnp.pad(doc_ids.astype(BF16), ((0, 0), (0, lanes - rows))),
        ],
        axis=0,
    )
    packs = [pack]
    for r in range(1, seq):
        pairs = [(i, (i + r) % seq) for i in range(seq)]
        packs.append(lax.ppermute(pack, "seq", pairs))

    x = layer_input[0]
    got = []
    for o in range(cells):
        piece = lax.dynamic_slice_in_dim(x, (cell ^ o) * 2 * size, 2 * size, 1)
        if o:
            piece = lax.ppermute(piece, both, swap_pairs(plane, member(o, 0)))
        got.append(piece)
    got = jnp.concatenate(got, axis=0)
    mine = lax.dynamic_slice_in_dim(got, core * size, size, 1)
    theirs = lax.dynamic_slice_in_dim(got, (1 - core) * size, size, 1)
    x_plane = jnp.concatenate([mine, core_swap(theirs)], axis=0)

    own_slice = (cell * 2 + core) * size
    w_slice = jnp.concatenate(
        [lax.dynamic_slice_in_dim(w, own_slice, size, 0) for w in (key_proj, value_proj)], axis=1
    )
    w_slots = line_exchange(w_slice)
    x_slots = line_exchange(x_plane)
    at = scalars(z, cell, core, s)

    query_grad, own_terms, *prev_terms = attention(at, queries[0], out_grad[0], packs)
    terms = []
    for r in range(1, seq):
        pairs = [(i, (i - r) % seq) for i in range(seq)]
        terms.append(lax.ppermute(prev_terms[r - 1], "seq", pairs))
    dkv = sum([t.astype(F32) for t in terms], own_terms).astype(BF16)

    pieces = [lax.dynamic_slice_in_dim(dkv, z * sub, sub, 0)]
    for r in range(1, heads):
        piece = lax.dynamic_slice_in_dim(dkv, (z ^ r) * sub, sub, 0)
        pieces.append(lax.ppermute(piece, "head", swap_pairs(heads, r)))
    head_rows = cell_gather(jnp.concatenate(pieces, axis=1))

    dkv_own = jnp.stack(cell_gather(dkv))
    dkv_other = core_swap(dkv_own)
    both_rows = []
    for r in range(heads):
        halves = [
            lax.dynamic_slice_in_dim(t, (z ^ r) * sub, sub, 1).reshape(cells * sub, 2 * HD)
            for t in (dkv_own, dkv_other)
        ]
        both_rows.append(jnp.concatenate(halves, axis=0))
    outer = (z == 0) | (z == heads - 1)

    if len(x_slots) > heads:
        x_slots = x_slots[: heads - 1] + [jnp.where(outer, x_slots[heads], x_slots[heads - 1])]
    grad = sum(dot(x_slots[r], both_rows[r], 0, 0) for r in range(heads)).astype(BF16)
    grad_own = cell_gather(grad)
    items = [(o, 0, g) for o, g in enumerate(grad_own)]
    items += [(o, 1, core_swap(g)) for o, g in enumerate(grad_own)]
    outs = spread(at, d_model, [i for i in items if i[0] == 0])

    if len(w_slots) > heads:
        w_slots = w_slots[: heads - 1] + [jnp.where(outer, w_slots[heads], w_slots[heads - 1])]
    w_own = jnp.stack(w_slots)
    parts = list(input_parts(w_own, core_swap(w_own), head_rows))
    for o in far_first(cells):
        parts[o] = lax.ppermute(parts[o], both, swap_pairs(plane, member(o, 0)))
    rest = [i for i in items if i[0]]
    if size % HD:
        grad_keyproj, grad_valueproj = spread(at, d_model, rest, outs)
        input_grad = place(at, parts)
    else:
        grad_keyproj, grad_valueproj, input_grad = spread(at, d_model, rest, outs, parts)
    return query_grad[None], input_grad[None], grad_keyproj, grad_valueproj


def solution(mesh):
    return jax.shard_map(
        shards,
        mesh=mesh,
        in_specs=(
            P("dp", "seq", "head"),
            P("dp", "seq", "head"),
            P("dp", "seq", "head"),
            P("dp", "seq", "head"),
            P("dp", "seq"),
            P("dp", ("seq", "head"), None),
            P(None, "head"),
            P(None, "head"),
        ),
        out_specs=(
            P("dp", "seq", "head"),
            P("dp", ("seq", "head"), None),
            P(None, "head"),
            P(None, "head"),
        ),
        check_vma=False,
    )
```

```python
import functools

import jax
import jax.numpy as jnp
from jax import lax
from jax.experimental import pallas as pl
from jax.experimental.pallas import tpu as pltpu
from jax.sharding import PartitionSpec as P

HD = 128
MASKED = -1e30
F32 = jnp.float32
BF16 = jnp.bfloat16
VMEM = pl.BlockSpec(memory_space=pltpu.VMEM)
SMEM = pl.BlockSpec(memory_space=pltpu.SMEM)
ANY = pl.BlockSpec(memory_space=pl.ANY)


def dot(a, b, ca, cb):
    return lax.dot_general(a, b, (((ca,), (cb,)), ((), ())), preferred_element_type=F32)


def scalars(*values):
    return jnp.stack([jnp.asarray(v, jnp.int32) for v in values])


def attention_kernel(blocks, group, at_ref, q_ref, g_ref, *refs):
    kv_refs, refs = refs[:blocks], refs[blocks:]
    dq_ref, own_ref, *prev_refs = refs
    rows = q_ref.shape[0]
    k_refs = [ref.at[:rows, :HD] for ref in kv_refs]
    v_refs = [ref.at[:rows, HD:] for ref in kv_refs]
    doc_refs = [ref.at[rows:, :rows] for ref in kv_refs]
    scale = HD**-0.5
    query_doc = doc_refs[0][...].astype(F32)
    allowed = []
    for b in range(blocks):
        key_doc = doc_refs[b][...].astype(F32)
        if b:
            key_doc = jnp.where(at_ref[3] >= b, key_doc, -1.0)
        same = jnp.broadcast_to(key_doc, (HD, rows)).T[:, :1] == query_doc
        if b == 0:
            key_pos = lax.broadcasted_iota(jnp.int32, (rows, rows), 0)
            query_pos = lax.broadcasted_iota(jnp.int32, (rows, rows), 1)
            same = same & (key_pos <= query_pos)
        allowed.append(same)
    dk = [jnp.zeros((rows, HD), F32) for _ in range(blocks)]
    dv = [jnp.zeros((rows, HD), F32) for _ in range(blocks)]
    for h in range(group):
        cols = slice(h * HD, (h + 1) * HD)
        q, g = q_ref[:, cols], g_ref[:, cols]
        scores = [
            jnp.where(allowed[b], dot(k_refs[b][...], q, 1, 1) * scale, MASKED)
            for b in range(blocks)
        ]
        top = functools.reduce(jnp.maximum, [jnp.max(x, axis=0, keepdims=True) for x in scores])
        parts = [jnp.exp(x - top) for x in scores]
        total = sum(jnp.sum(x, axis=0, keepdims=True) for x in parts)
        inverse = 1.0 / total
        weights = [x * inverse for x in parts]
        wgrads = [dot(v_refs[b][...], g, 1, 1) for b in range(blocks)]
        delta = sum(jnp.sum(w * d, axis=0, keepdims=True) for w, d in zip(weights, wgrads))
        dq = jnp.zeros((rows, HD), F32)
        for b in range(blocks):
            ds = (weights[b] * (wgrads[b] - delta) * scale).astype(BF16)
            dq += dot(ds, k_refs[b][...], 0, 0)
            dk[b] += dot(ds, q, 1, 0)
            dv[b] += dot(weights[b].astype(BF16), g, 1, 0)
        dq_ref[:, cols] = dq.astype(BF16)
    own_ref[:, :HD] = dk[0]
    own_ref[:, HD:] = dv[0]
    for b in range(1, blocks):
        prev_refs[b - 1][:, :HD] = dk[b].astype(BF16)
        prev_refs[b - 1][:, HD:] = dv[b].astype(BF16)


def attention(at, q, g, packs):
    rows, width = q.shape
    blocks = len(packs)
    outs = [
        jax.ShapeDtypeStruct((rows, width), BF16),
        jax.ShapeDtypeStruct((rows, 2 * HD), F32),
    ] + [jax.ShapeDtypeStruct((rows, 2 * HD), BF16)] * (blocks - 1)
    return pl.pallas_call(
        functools.partial(attention_kernel, blocks, width // HD),
        out_shape=outs,
        in_specs=[SMEM] + [VMEM] * (2 + blocks),
        name="attention",
        cost_estimate=pl.CostEstimate(
            flops=10 * rows * rows * blocks * width,
            transcendentals=rows * rows * blocks * width // HD,
            bytes_accessed=8 * rows * width,
        ),
    )(at, q, g, *packs)


def place(at, pieces):
    cells, (sub, slab) = len(pieces), pieces[0].shape
    out = jnp.zeros((sub, slab * cells), BF16)
    for o, piece in enumerate(pieces):
        for j, half in enumerate(jnp.split(piece, 2, axis=1)):
            start = ((at[1] ^ o) * 2 + (at[2] ^ j)) * (slab // 2)
            out = lax.dynamic_update_slice_in_dim(out, half, start, 1)
    return out


def spread_kernel(places, parts, at_ref, *refs):
    pieces, refs = refs[: len(places)], refs[len(places) :]
    part_refs, (key_ref, value_ref, *placed, key_buf, value_buf, sems) = refs[:parts], refs[-6:]
    if not parts:
        key_ref, value_ref = refs[-5:-3]
    size = pieces[0].shape[0]
    waits = []
    for i, ((o, flip), piece) in enumerate(zip(places, pieces)):
        base = pl.multiple_of(((at_ref[1] ^ o) * 2 + (at_ref[2] ^ flip)) * size, 8)
        for n, (out_ref, buf) in enumerate(((key_ref, key_buf), (value_ref, value_buf))):
            buf[i] = piece[:, n * HD : (n + 1) * HD].astype(F32)
            copy = pltpu.make_async_copy(
                buf.at[i], out_ref.at[pl.ds(base, size), :], sems.at[n, i]
            )
            copy.start()
            waits.append(copy)
    for o, ref in enumerate(part_refs):
        for j in range(2):
            start = pl.multiple_of(((at_ref[1] ^ o) * 2 + (at_ref[2] ^ j)) * size, HD)
            placed[0][:, pl.ds(start, size)] = ref[:, j * size : (j + 1) * size]
    for copy in waits:
        copy.wait()


def spread(at, total, items, outs=(), parts=()):
    count, size = len(items), items[0][2].shape[0]
    shapes = [jax.ShapeDtypeStruct((total, HD), F32)] * 2
    buf = pltpu.VMEM((count, size, HD), F32)
    specs = [ANY, ANY]
    if parts:
        shapes.append(jax.ShapeDtypeStruct((parts[0].shape[0], total), BF16))
        specs.append(VMEM)
    first = 1 + count + len(parts)
    return pl.pallas_call(
        functools.partial(spread_kernel, tuple(item[:2] for item in items), len(parts)),
        out_shape=shapes,
        in_specs=[SMEM] + [VMEM] * (count + len(parts)) + [ANY] * len(outs),
        out_specs=specs,
        scratch_shapes=[buf, buf, pltpu.SemaphoreType.DMA((2, count))],
        input_output_aliases={first + n: n for n in range(len(outs))},
    )(at, *[item[2] for item in items], *parts, *outs)


def swap_pairs(n, m):
    return [(i, i ^ m) for i in range(n)]


def far_first(count):
    return sorted(range(1, count), key=lambda m: (-bin(m).count("1"), -m))


def line_exchange(x):
    n = lax.axis_size("head")
    slots = {0: x}
    for r in head_offsets(n):
        pairs = swap_pairs(n, r)
        if n == 4 and r == 3:
            pairs = [(0, 0), (1, 2), (2, 1), (3, 3)]
        slots[r] = lax.ppermute(x, "head", pairs)
    out = [slots[r] for r in range(n)]
    if n == 4:
        out.append(lax.ppermute(slots[2], "head", swap_pairs(n, 1)))
    return out


def head_offsets(n):
    return [2, 1, 3] if n == 4 else list(range(1, n))


def shards(queries, key_cache, value_cache, out_grad, doc_ids, layer_input, key_proj, value_proj):
    dp, seq, heads = (lax.axis_size(a) for a in ("dp", "seq", "head"))
    d, s, z = (lax.axis_index(a) for a in ("dp", "seq", "head"))
    plane, cells = dp * seq, dp // 2 * seq
    core, cell = d % 2, d // 2 * seq + s
    rows, _ = queries.shape[1:]
    d_model = layer_input.shape[2]
    size = d_model // plane
    sub = rows // heads
    both = ("dp", "seq")

    def member(o, c):
        return (o // seq * 2 + c) * seq + o % seq

    def cell_gather(x):
        got = {0: x}
        for o in far_first(cells):
            got[o] = lax.ppermute(x, both, swap_pairs(plane, member(o, 0)))
        return [got[o] for o in range(cells)]

    def core_swap(x):
        return lax.ppermute(x, "dp", swap_pairs(dp, 1))

    pack = jnp.concatenate([key_cache[0], value_cache[0]], axis=1)
    lanes = max(rows, 2 * HD)
    pack = jnp.concatenate(
        [
            jnp.pad(pack, ((0, 0), (0, lanes - 2 * HD))),
            jnp.pad(doc_ids.astype(BF16), ((0, 0), (0, lanes - rows))),
        ],
        axis=0,
    )
    packs = [pack]
    for r in range(1, seq):
        pairs = [(i, (i + r) % seq) for i in range(seq)]
        packs.append(lax.ppermute(pack, "seq", pairs))

    x = layer_input[0]
    got = []
    for o in range(cells):
        piece = lax.dynamic_slice_in_dim(x, (cell ^ o) * 2 * size, 2 * size, 1)
        if o:
            piece = lax.ppermute(piece, both, swap_pairs(plane, member(o, 0)))
        got.append(piece)
    got = jnp.concatenate(got, axis=0)
    mine = lax.dynamic_slice_in_dim(got, core * size, size, 1)
    theirs = lax.dynamic_slice_in_dim(got, (1 - core) * size, size, 1)
    x_plane = jnp.concatenate([mine, core_swap(theirs)], axis=0)

    own_slice = (cell * 2 + core) * size
    w_slice = jnp.concatenate(
        [lax.dynamic_slice_in_dim(w, own_slice, size, 0) for w in (key_proj, value_proj)], axis=1
    )
    w_slots = line_exchange(w_slice)
    x_slots = line_exchange(x_plane)
    at = scalars(z, cell, core, s)

    query_grad, own_terms, *prev_terms = attention(at, queries[0], out_grad[0], packs)
    terms = []
    for r in range(1, seq):
        pairs = [(i, (i - r) % seq) for i in range(seq)]
        terms.append(lax.ppermute(prev_terms[r - 1], "seq", pairs))
    dkv = sum([t.astype(F32) for t in terms], own_terms).astype(BF16)

    pieces = [lax.dynamic_slice_in_dim(dkv, z * sub, sub, 0)]
    for r in range(1, heads):
        piece = lax.dynamic_slice_in_dim(dkv, (z ^ r) * sub, sub, 0)
        pieces.append(lax.ppermute(piece, "head", swap_pairs(heads, r)))
    pieces = jnp.concatenate(pieces, axis=1)
    head_rows = cell_gather(pieces)

    dkv_own = jnp.stack(cell_gather(dkv))
    dkv_other = core_swap(dkv_own)
    both_rows = []
    for r in range(heads):
        halves = [
            lax.dynamic_slice_in_dim(t, (z ^ r) * sub, sub, 1).reshape(cells * sub, 2 * HD)
            for t in (dkv_own, dkv_other)
        ]
        both_rows.append(jnp.concatenate(halves, axis=0))
    outer = (z == 0) | (z == heads - 1)

    if len(x_slots) > heads:
        x_slots = x_slots[: heads - 1] + [jnp.where(outer, x_slots[heads], x_slots[heads - 1])]
    grad = sum(dot(x_slots[r], both_rows[r], 0, 0) for r in range(heads)).astype(BF16)
    grad_own = cell_gather(grad)
    items = [(o, 0, g) for o, g in enumerate(grad_own)]
    items += [(o, 1, core_swap(g)) for o, g in enumerate(grad_own)]
    outs = spread(at, d_model, [i for i in items if i[0] == 0])

    if len(w_slots) > heads:
        w_slots = w_slots[: heads - 1] + [jnp.where(outer, w_slots[heads], w_slots[heads - 1])]
    w_own = jnp.concatenate(w_slots, axis=1)
    w_both = jnp.concatenate([w_own, core_swap(w_own)], axis=0)
    parts = [dot(t, w_both, 1, 1).astype(BF16) for t in head_rows]
    for o in far_first(cells):
        parts[o] = lax.ppermute(parts[o], both, swap_pairs(plane, member(o, 0)))
    rest = [i for i in items if i[0]]
    if size % HD:
        grad_keyproj, grad_valueproj = spread(at, d_model, rest, outs)
        input_grad = place(at, parts)
    else:
        grad_keyproj, grad_valueproj, input_grad = spread(at, d_model, rest, outs, parts)
    return query_grad[None], input_grad[None], grad_keyproj, grad_valueproj


def solution(mesh):
    return jax.shard_map(
        shards,
        mesh=mesh,
        in_specs=(
            P("dp", "seq", "head"),
            P("dp", "seq", "head"),
            P("dp", "seq", "head"),
            P("dp", "seq", "head"),
            P("dp", "seq"),
            P("dp", ("seq", "head"), None),
            P(None, "head"),
            P(None, "head"),
        ),
        out_specs=(
            P("dp", "seq", "head"),
            P("dp", ("seq", "head"), None),
            P(None, "head"),
            P(None, "head"),
        ),
        check_vma=False,
    )
```

```python
import functools

import jax
import jax.numpy as jnp
from jax import lax
from jax.experimental import pallas as pl
from jax.experimental.pallas import tpu as pltpu
from jax.sharding import PartitionSpec as P

HD = 128
MASKED = -1e30
F32 = jnp.float32
BF16 = jnp.bfloat16
VMEM = pl.BlockSpec(memory_space=pltpu.VMEM)
SMEM = pl.BlockSpec(memory_space=pltpu.SMEM)
ANY = pl.BlockSpec(memory_space=pl.ANY)


def dot(a, b, ca, cb):
    return lax.dot_general(a, b, (((ca,), (cb,)), ((), ())), preferred_element_type=F32)


def scalars(*values):
    return jnp.stack([jnp.asarray(v, jnp.int32) for v in values])


def attention_kernel(blocks, group, at_ref, q_ref, g_ref, *refs):
    kv_refs, refs = refs[:blocks], refs[blocks:]
    dq_ref, own_ref, *prev_refs = refs
    rows = q_ref.shape[0]
    k_refs = [ref.at[:rows, :HD] for ref in kv_refs]
    v_refs = [ref.at[:rows, HD:] for ref in kv_refs]
    doc_refs = [ref.at[rows:, :rows] for ref in kv_refs]
    scale = HD**-0.5
    query_doc = doc_refs[0][...].astype(F32)
    allowed = []
    for b in range(blocks):
        key_doc = doc_refs[b][...].astype(F32)
        if b:
            key_doc = jnp.where(at_ref[3] >= b, key_doc, -1.0)
        same = jnp.broadcast_to(key_doc, (HD, rows)).T[:, :1] == query_doc
        if b == 0:
            key_pos = lax.broadcasted_iota(jnp.int32, (rows, rows), 0)
            query_pos = lax.broadcasted_iota(jnp.int32, (rows, rows), 1)
            same = same & (key_pos <= query_pos)
        allowed.append(same)
    dk = [jnp.zeros((rows, HD), F32) for _ in range(blocks)]
    dv = [jnp.zeros((rows, HD), F32) for _ in range(blocks)]
    for h in range(group):
        cols = slice(h * HD, (h + 1) * HD)
        q, g = q_ref[:, cols], g_ref[:, cols]
        scores = [
            jnp.where(allowed[b], dot(k_refs[b][...], q, 1, 1) * scale, MASKED)
            for b in range(blocks)
        ]
        top = functools.reduce(jnp.maximum, [jnp.max(x, axis=0, keepdims=True) for x in scores])
        parts = [jnp.exp(x - top) for x in scores]
        total = sum(jnp.sum(x, axis=0, keepdims=True) for x in parts)
        inverse = 1.0 / total
        weights = [x * inverse for x in parts]
        wgrads = [dot(v_refs[b][...], g, 1, 1) for b in range(blocks)]
        delta = sum(jnp.sum(w * d, axis=0, keepdims=True) for w, d in zip(weights, wgrads))
        dq = jnp.zeros((rows, HD), F32)
        for b in range(blocks):
            ds = (weights[b] * (wgrads[b] - delta) * scale).astype(BF16)
            dq += dot(ds, k_refs[b][...], 0, 0)
            dk[b] += dot(ds, q, 1, 0)
            dv[b] += dot(weights[b].astype(BF16), g, 1, 0)
        dq_ref[:, cols] = dq.astype(BF16)
    own_ref[:, :HD] = dk[0]
    own_ref[:, HD:] = dv[0]
    for b in range(1, blocks):
        prev_refs[b - 1][:, :HD] = dk[b].astype(BF16)
        prev_refs[b - 1][:, HD:] = dv[b].astype(BF16)


def attention(at, q, g, packs):
    rows, width = q.shape
    blocks = len(packs)
    outs = [
        jax.ShapeDtypeStruct((rows, width), BF16),
        jax.ShapeDtypeStruct((rows, 2 * HD), F32),
    ] + [jax.ShapeDtypeStruct((rows, 2 * HD), BF16)] * (blocks - 1)
    return pl.pallas_call(
        functools.partial(attention_kernel, blocks, width // HD),
        out_shape=outs,
        in_specs=[SMEM] + [VMEM] * (2 + blocks),
        name="attention",
        cost_estimate=pl.CostEstimate(
            flops=10 * rows * rows * blocks * width,
            transcendentals=rows * rows * blocks * width // HD,
            bytes_accessed=8 * rows * width,
        ),
    )(at, q, g, *packs)


def place(at, pieces):
    cells, (sub, slab) = len(pieces), pieces[0].shape
    out = jnp.zeros((sub, slab * cells), BF16)
    for o, piece in enumerate(pieces):
        for j, half in enumerate(jnp.split(piece, 2, axis=1)):
            start = ((at[1] ^ o) * 2 + (at[2] ^ j)) * (slab // 2)
            out = lax.dynamic_update_slice_in_dim(out, half, start, 1)
    return out


def spread_kernel(places, parts, at_ref, *refs):
    pieces, refs = refs[: len(places)], refs[len(places) :]
    part_refs, (key_ref, value_ref, *placed, key_buf, value_buf, sems) = refs[:parts], refs[-6:]
    if not parts:
        key_ref, value_ref = refs[-5:-3]
    size = pieces[0].shape[0]
    waits = []
    for i, ((o, flip), piece) in enumerate(zip(places, pieces)):
        base = pl.multiple_of(((at_ref[1] ^ o) * 2 + (at_ref[2] ^ flip)) * size, 8)
        for n, (out_ref, buf) in enumerate(((key_ref, key_buf), (value_ref, value_buf))):
            buf[i] = piece[:, n * HD : (n + 1) * HD].astype(F32)
            copy = pltpu.make_async_copy(
                buf.at[i], out_ref.at[pl.ds(base, size), :], sems.at[n, i]
            )
            copy.start()
            waits.append(copy)
    for o, ref in enumerate(part_refs):
        for j in range(2):
            start = pl.multiple_of(((at_ref[1] ^ o) * 2 + (at_ref[2] ^ j)) * size, HD)
            placed[0][:, pl.ds(start, size)] = ref[:, j * size : (j + 1) * size]
    for copy in waits:
        copy.wait()


def spread(at, total, items, outs=(), parts=()):
    count, size = len(items), items[0][2].shape[0]
    shapes = [jax.ShapeDtypeStruct((total, HD), F32)] * 2
    buf = pltpu.VMEM((count, size, HD), F32)
    specs = [ANY, ANY]
    if parts:
        shapes.append(jax.ShapeDtypeStruct((parts[0].shape[0], total), BF16))
        specs.append(VMEM)
    first = 1 + count + len(parts)
    return pl.pallas_call(
        functools.partial(spread_kernel, tuple(item[:2] for item in items), len(parts)),
        out_shape=shapes,
        in_specs=[SMEM] + [VMEM] * (count + len(parts)) + [ANY] * len(outs),
        out_specs=specs,
        scratch_shapes=[buf, buf, pltpu.SemaphoreType.DMA((2, count))],
        input_output_aliases={first + n: n for n in range(len(outs))},
    )(at, *[item[2] for item in items], *parts, *outs)


def swap_pairs(n, m):
    return [(i, i ^ m) for i in range(n)]


def far_first(count):
    return sorted(range(1, count), key=lambda m: (-bin(m).count("1"), -m))


def line_exchange(x):
    n = lax.axis_size("head")
    slots = {0: x}
    for r in head_offsets(n):
        pairs = swap_pairs(n, r)
        if n == 4 and r == 3:
            pairs = [(0, 0), (1, 2), (2, 1), (3, 3)]
        slots[r] = lax.ppermute(x, "head", pairs)
    out = [slots[r] for r in range(n)]
    if n == 4:
        out.append(lax.ppermute(slots[2], "head", swap_pairs(n, 1)))
    return out


def head_offsets(n):
    return [2, 1, 3] if n == 4 else list(range(1, n))


def shards(queries, key_cache, value_cache, out_grad, doc_ids, layer_input, key_proj, value_proj):
    dp, seq, heads = (lax.axis_size(a) for a in ("dp", "seq", "head"))
    d, s, z = (lax.axis_index(a) for a in ("dp", "seq", "head"))
    plane, cells = dp * seq, dp // 2 * seq
    core, cell = d % 2, d // 2 * seq + s
    rows, _ = queries.shape[1:]
    d_model = layer_input.shape[2]
    size = d_model // plane
    sub = rows // heads
    both = ("dp", "seq")

    def member(o, c):
        return (o // seq * 2 + c) * seq + o % seq

    def cell_gather(x):
        got = {0: x}
        for o in far_first(cells):
            got[o] = lax.ppermute(x, both, swap_pairs(plane, member(o, 0)))
        return [got[o] for o in range(cells)]

    def core_swap(x):
        return lax.ppermute(x, "dp", swap_pairs(dp, 1))

    pack = jnp.concatenate([key_cache[0], value_cache[0]], axis=1)
    lanes = max(rows, 2 * HD)
    pack = jnp.concatenate(
        [
            jnp.pad(pack, ((0, 0), (0, lanes - 2 * HD))),
            jnp.pad(doc_ids.astype(BF16), ((0, 0), (0, lanes - rows))),
        ],
        axis=0,
    )
    packs = [pack]
    for r in range(1, seq):
        pairs = [(i, (i + r) % seq) for i in range(seq)]
        packs.append(lax.ppermute(pack, "seq", pairs))

    x = layer_input[0]
    got = []
    for o in range(cells):
        piece = lax.dynamic_slice_in_dim(x, (cell ^ o) * 2 * size, 2 * size, 1)
        if o:
            piece = lax.ppermute(piece, both, swap_pairs(plane, member(o, 0)))
        got.append(piece)
    got = jnp.concatenate(got, axis=0)
    mine = lax.dynamic_slice_in_dim(got, core * size, size, 1)
    theirs = lax.dynamic_slice_in_dim(got, (1 - core) * size, size, 1)
    x_plane = jnp.concatenate([mine, core_swap(theirs)], axis=0)

    own_slice = (cell * 2 + core) * size
    w_slice = jnp.concatenate(
        [lax.dynamic_slice_in_dim(w, own_slice, size, 0) for w in (key_proj, value_proj)], axis=1
    )
    w_slots = line_exchange(lax.optimization_barrier(w_slice))
    x_slots = line_exchange(x_plane)
    at = scalars(z, cell, core, s)

    query_grad, own_terms, *prev_terms = attention(at, queries[0], out_grad[0], packs)
    terms = []
    for r in range(1, seq):
        pairs = [(i, (i - r) % seq) for i in range(seq)]
        terms.append(lax.ppermute(prev_terms[r - 1], "seq", pairs))
    dkv = sum([t.astype(F32) for t in terms], own_terms).astype(BF16)

    pieces = [lax.dynamic_slice_in_dim(dkv, z * sub, sub, 0)]
    for r in range(1, heads):
        piece = lax.dynamic_slice_in_dim(dkv, (z ^ r) * sub, sub, 0)
        pieces.append(lax.ppermute(piece, "head", swap_pairs(heads, r)))
    pieces = jnp.concatenate(pieces, axis=1)
    head_rows = cell_gather(pieces)

    gathered = cell_gather(dkv)
    dkv_own = jnp.stack(gathered)
    dkv_other = core_swap(dkv_own)
    both_rows = []
    for r in range(heads):
        halves = [
            lax.dynamic_slice_in_dim(t, (z ^ r) * sub, sub, 1).reshape(cells * sub, 2 * HD)
            for t in (dkv_own, dkv_other)
        ]
        both_rows.append(jnp.concatenate(halves, axis=0))
    outer = (z == 0) | (z == heads - 1)

    if len(x_slots) > heads:
        x_slots = x_slots[: heads - 1] + [jnp.where(outer, x_slots[heads], x_slots[heads - 1])]
    grad = sum(dot(x_slots[r], both_rows[r], 0, 0) for r in range(heads)).astype(BF16)
    grad_own = cell_gather(grad)
    items = [(o, 0, g) for o, g in enumerate(grad_own)]
    items += [(o, 1, core_swap(g)) for o, g in enumerate(grad_own)]
    outs = spread(at, d_model, [i for i in items if i[0] == 0])

    if len(w_slots) > heads:
        w_slots = w_slots[: heads - 1] + [jnp.where(outer, w_slots[heads], w_slots[heads - 1])]
    w_own = jnp.concatenate(w_slots, axis=1)
    w_other = core_swap(w_own)
    w_both = jnp.concatenate([w_own, w_other], axis=0)
    parts = [dot(t, w_both, 1, 1).astype(BF16) for t in head_rows]
    for o in far_first(cells):
        parts[o] = lax.ppermute(parts[o], both, swap_pairs(plane, member(o, 0)))
    rest = [i for i in items if i[0]]
    if size % HD:
        grad_keyproj, grad_valueproj = spread(at, d_model, rest, outs)
        input_grad = place(at, parts)
    else:
        grad_keyproj, grad_valueproj, input_grad = spread(at, d_model, rest, outs, parts)
    return query_grad[None], input_grad[None], grad_keyproj, grad_valueproj


def solution(mesh):
    return jax.shard_map(
        shards,
        mesh=mesh,
        in_specs=(
            P("dp", "seq", "head"),
            P("dp", "seq", "head"),
            P("dp", "seq", "head"),
            P("dp", "seq", "head"),
            P("dp", "seq"),
            P("dp", ("seq", "head"), None),
            P(None, "head"),
            P(None, "head"),
        ),
        out_specs=(
            P("dp", "seq", "head"),
            P("dp", ("seq", "head"), None),
            P(None, "head"),
            P(None, "head"),
        ),
        check_vma=False,
    )
```
